32 devices in a mesh: ta: 4 (over y, core), ha: 2 (over x), wa: 4 (over z).
Axes of the slice: x: 2, y: 2, z: 4, core: 2. Of those that a mesh axis runs over, the one named last changes fastest.
Arguments:
- latent: bfloat16 [16, 32, 128, 256], P('ta', 'ha', 'wa'), may hold values from -6 to 6
- kernel: bfloat16 [27, 256, 256], replicated, may hold values from -0.078125 to 0.078125
- bias: float32 [256], replicated, may hold values from -3 to 3
- cotangent: bfloat16 [16, 32, 128, 256], P('ta', 'ha', 'wa'), may hold values from -6 to 6
Outputs:
- activation: bfloat16 [16, 32, 128, 256], P('ta', 'ha', 'wa')
- latent_grad: bfloat16 [16, 32, 128, 256], P('ta', 'ha', 'wa')
- kernel_grad: float32 [27, 256, 256], replicated
- bias_grad: float32 [256], replicated
The draws below stay inside these ranges and needn't reach their ends.
All inputs are finite; a program needn't handle non-finite values.
Results may differ from the reference program's by a relative error of at most 0.0055.
Values may be sent and summed in bfloat16 or wider, within the bound.
A program may use at most 128 MiB of HBM per device.

```python
import jax
import jax.numpy as jnp
from jax import lax

C = 256
NT = 16
NH = 32
NW = 128


def block_levels(rng, shape, cuts, low, top_value):
    level, own = 1.0, jax.random.fold_in(rng, 6)
    for dim, parts in cuts:
        heights = jnp.exp(jax.random.uniform(jax.random.fold_in(own, dim), (parts,), jnp.float32, low / len(cuts), top_value / len(cuts)))
        level = level * jnp.repeat(heights, shape[dim] // parts).reshape([-1 if axis == dim else 1 for axis in range(len(shape))])
    return level


def noise(own_key, dims, scale, reach, split=(), held_as=jnp.bfloat16):
    drawn = jax.random.normal(own_key, dims, jnp.float32) * scale
    if len(split) > 0:
        drawn = block_levels(own_key, dims, split, -0.22, 0.18) * drawn
    return jnp.clip(drawn, min=-reach, max=reach).astype(held_as)


def setup_inputs(seed: int = 0) -> dict:
    key_of = jax.random.split(jax.random.key(seed), 5)
    latent = noise(key_of[0], (NT, NH, NW, C), 1.0, 6.0, ((0, 4), (1, 2), (2, 4)))
    kernel = noise(key_of[1], (27, C, C), (27 * C) ** -0.5, 0.078125)
    bias = noise(key_of[2], (C,), 0.5, 3.0, (), jnp.float32)
    cotangent = noise(key_of[3], (NT, NH, NW, C), 1.0, 6.0, ((0, 4), (1, 2), (2, 4)))
    return {"latent": latent, "kernel": kernel, "bias": bias, "cotangent": cotangent}


def convolve(padded, kernel, frames, rows, columns):
    width = kernel.shape[1]
    grouped = kernel.reshape(9, 3 * width, kernel.shape[2])
    total = jnp.zeros((frames * rows * columns, kernel.shape[2]), jnp.float32)
    for shift_t in range(3):
        for shift_h in range(3):
            pieces = [padded[shift_t:shift_t + frames, shift_h:shift_h + rows, shift_w:shift_w + columns] for shift_w in range(3)]
            columns_mat = jnp.concatenate(pieces, axis=-1).reshape(-1, 3 * width)
            total = total + jnp.dot(columns_mat, grouped[3 * shift_t + shift_h], preferred_element_type=jnp.float32)
    return total

def kernel_terms(padded, dflat, frames, rows, columns):
    width = padded.shape[-1]
    blocks = []
    for shift_t in range(3):
        for shift_h in range(3):
            pieces = [padded[shift_t:shift_t + frames, shift_h:shift_h + rows, shift_w:shift_w + columns] for shift_w in range(3)]
            columns_mat = jnp.concatenate(pieces, axis=-1).reshape(-1, 3 * width)
            blocks.append(lax.dot_general(columns_mat, dflat, (((0,), (0,)), ((), ())), preferred_element_type=jnp.float32))
    return jnp.stack(blocks).reshape(27, width, dflat.shape[1])

def flipped(kernel):
    width = kernel.shape[1]
    return kernel.reshape(3, 3, 3, width, width)[::-1, ::-1, ::-1].transpose(0, 1, 2, 4, 3).reshape(27, width, width)

def reference(latent, kernel, bias, cotangent):
    frames, rows, columns, width = latent.shape
    padded = jnp.pad(latent, ((2, 0), (1, 1), (1, 1), (0, 0)))
    pre = convolve(padded, kernel, frames, rows, columns) + bias[None, :]
    sig = jax.nn.sigmoid(pre)
    activation = (pre * sig).astype(jnp.bfloat16).reshape(frames, rows, columns, width)
    cot = cotangent.reshape(-1, width).astype(jnp.float32)
    dflat = (cot * sig * (1.0 + pre * (1.0 - sig))).astype(jnp.bfloat16)
    dpadded = jnp.pad(dflat.reshape(frames, rows, columns, width), ((0, 2), (1, 1), (1, 1), (0, 0)))
    latent_grad = convolve(dpadded, flipped(kernel), frames, rows, columns).astype(jnp.bfloat16).reshape(frames, rows, columns, width)
    scale = 1.0 / jnp.sqrt(jnp.float32(frames * rows * columns))
    kernel_grad = kernel_terms(padded, dflat, frames, rows, columns) * scale
    bias_grad = lax.optimization_barrier(jnp.sum(dflat.astype(jnp.float32), axis=0)) * scale
    return (activation, latent_grad, kernel_grad, bias_grad)
```

```python
import jax
import jax.numpy as jnp
from jax import lax
from jax.experimental import pallas as pl
from jax.experimental.pallas import tpu as pltpu
from jax.sharding import PartitionSpec as P

AXES = ("ta", "ha", "wa")


def with_halo(block, sides, width):
    for axis, dim in sides:
        count = lax.axis_size(axis)
        forward = [(i, i + 1) for i in range(count - 1)]
        backward = [(target, source) for source, target in forward]
        low = lax.ppermute(
            lax.slice_in_dim(block, block.shape[dim] - width, None, axis=dim), axis, forward
        )
        high = lax.ppermute(lax.slice_in_dim(block, 0, width, axis=dim), axis, backward)
        block = jnp.concatenate([low, block, high], axis=dim)
    return block


def shifted(block, axis, distance):
    devices = range(lax.axis_size(axis))
    route = [(i - distance, i) for i in devices if i - distance in devices]
    return lax.ppermute(block, axis, route)


def bordered_latent(latent):
    framed = with_halo(latent, (("ha", 1), ("wa", 2)), 1)
    earlier = shifted(framed[-2:], "ta", 1)
    return jnp.concatenate([earlier, framed], axis=0)


def bordered_grad(dfield):
    framed = with_halo(dfield, (("ha", 1), ("wa", 2)), 1)
    later = shifted(framed[:2], "ta", -1)
    return jnp.concatenate([framed, later], axis=0)


def gather_taps(padded_ref, taps_ref, rows, columns, width):
    def frame(f, carry):
        for c in range(3):
            moved = padded_ref[f, :, c : c + columns, :]
            for b in range(3):
                at = (3 * b + c) * width
                taps_ref[f, :, :, at : at + width] = moved[b : b + rows]
        return carry

    lax.fori_loop(0, padded_ref.shape[0], frame, 0)


def forward_kernel(
    padded_ref, kernel_ref, bias_ref, cot_ref, act_ref, dpre_ref, kgrad_ref, bgrad_ref, taps_ref, dturn_ref
):
    frames, rows, columns, width = cot_ref.shape
    cells = rows * columns
    gather_taps(padded_ref, taps_ref, rows, columns, width)
    bgrad_ref[...] = jnp.zeros_like(bgrad_ref)
    for t in range(frames):
        pre = bias_ref[...]
        for a in range(3):
            pre = pre + jnp.dot(
                taps_ref[t + a].reshape(cells, 9 * width),
                kernel_ref[a],
                preferred_element_type=jnp.float32,
            )
        sig = jax.nn.sigmoid(pre)
        act_ref[t] = (pre * sig).astype(jnp.bfloat16).reshape(rows, columns, width)
        cot = cot_ref[t].reshape(cells, width).astype(jnp.float32)
        dpre = (cot * sig * (1.0 + pre * (1.0 - sig))).astype(jnp.bfloat16)
        dpre_ref[t] = dpre.reshape(rows, columns, width)
        wide = dpre.astype(jnp.float32)
        bgrad_ref[...] += jnp.sum(wide, axis=0, keepdims=True)
        dturn_ref[:, t * cells : (t + 1) * cells] = wide.T.astype(jnp.bfloat16)
    for a in range(3):
        for g in range(9):
            kgrad_ref[a, g] = jnp.dot(
                dturn_ref[...],
                taps_ref[a : a + frames, :, :, g * width : (g + 1) * width].reshape(frames * cells, width),
                preferred_element_type=jnp.float32,
            ).astype(kgrad_ref.dtype)


def backward_kernel(padded_ref, kernel_ref, out_ref, taps_ref, turned_ref):
    frames, rows, columns, width = out_ref.shape
    cells = rows * columns
    gather_taps(padded_ref, taps_ref, rows, columns, width)
    for a in range(3):
        for g in range(9):
            turned_ref[a, :, g * width : (g + 1) * width] = kernel_ref[26 - (9 * a + g)]
    for t in range(frames):
        total = None
        for a in range(3):
            part = lax.dot_general(
                taps_ref[t + a].reshape(cells, 9 * width),
                turned_ref[a],
                (((1,), (1,)), ((), ())),
                preferred_element_type=jnp.float32,
            )
            total = part if total is None else total + part
        out_ref[t] = total.astype(jnp.bfloat16).reshape(rows, columns, width)


def whole(n):
    return [pl.BlockSpec(memory_space=pltpu.VMEM)] * n


def shards(latent, kernel, bias, cotangent):
    frames, rows, columns, width = latent.shape
    cells = frames * rows * columns
    flops = 2 * cells * 27 * width * width
    field = jax.ShapeDtypeStruct(latent.shape, jnp.bfloat16)
    taps = pltpu.VMEM((frames + 2, rows, columns, 9 * width), jnp.bfloat16)
    params = pltpu.CompilerParams(vmem_limit_bytes=60 * 1024 * 1024)

    padded = bordered_latent(latent)
    activation, dpre, local_kernel, local_bias = pl.pallas_call(
        forward_kernel,
        out_shape=(
            field,
            field,
            jax.ShapeDtypeStruct((3, 9, width, width), jnp.bfloat16),
            jax.ShapeDtypeStruct((1, width), jnp.float32),
        ),
        in_specs=whole(4),
        out_specs=tuple(whole(4)),
        scratch_shapes=[taps, pltpu.VMEM((width, cells), jnp.bfloat16)],
        compiler_params=params,
        cost_estimate=pl.CostEstimate(flops=2 * flops, bytes_accessed=12 << 20, transcendentals=0),
    )(padded, kernel.reshape(3, 9 * width, width), bias[None, :], cotangent)

    scale = 1.0 / jnp.sqrt(
        jnp.float32(cells * lax.axis_size("ta") * lax.axis_size("ha") * lax.axis_size("wa"))
    )
    kernel_sum = lax.psum(local_kernel.reshape(27, width, width), AXES)
    bias_sum = lax.psum(local_bias[0], AXES)

    dpadded = bordered_grad(dpre)
    latent_grad = pl.pallas_call(
        backward_kernel,
        out_shape=field,
        in_specs=whole(2),
        out_specs=whole(1)[0],
        scratch_shapes=[taps, pltpu.VMEM((3, width, 9 * width), jnp.bfloat16)],
        compiler_params=params,
        cost_estimate=pl.CostEstimate(flops=flops, bytes_accessed=8 << 20, transcendentals=0),
    )(dpadded, kernel)

    kernel_grad = kernel_sum.astype(jnp.float32).transpose(0, 2, 1) * scale
    return (activation, latent_grad, kernel_grad, bias_sum * scale)


def solution(mesh):
    placed = (P("ta", "ha", "wa", None), P(), P(), P("ta", "ha", "wa", None))
    return jax.shard_map(
        shards,
        mesh=mesh,
        in_specs=placed,
        out_specs=(P("ta", "ha", "wa", None), P("ta", "ha", "wa", None), P(), P()),
        check_vma=False,
    )
```
